32 devices in a mesh: fsdp: 32 (over z, y, x, core), dp: 1.
Axes of the slice: x: 2, y: 2, z: 4, core: 2. Of those that a mesh axis runs over, the one named last changes fastest.
Arguments:
- inputs: bfloat16 [8192, 2560], P(('fsdp', 'dp')), may hold values from -6 to 6
- value_cotangent: bfloat16 [8192, 512], P(('fsdp', 'dp')), may hold values from -0.15625 to 0.15625
- master: float32 [2560, 4, 128], P('fsdp', None, 'dp'), may hold values from -0.125 to 0.125
- first_moment: float32 [2560, 4, 128], P('fsdp', None, 'dp'), may hold values from -6 to 6
- second_moment: float32 [2560, 4, 128], P('fsdp', None, 'dp'), may hold values from 0.25 to 4
Outputs:
- moment_one_new: float32 [2560, 4, 128], P('fsdp', None, 'dp')
- moment_two_new: float32 [2560, 4, 128], P('fsdp', None, 'dp')
- master_new: float32 [2560, 4, 128], P('fsdp', None, 'dp')
- head_blocks: bfloat16 [32, 2560, 128], P('fsdp', None, 'dp')
The draws below stay inside these ranges and needn't reach their ends.
All inputs are finite; a program needn't handle non-finite values.
Results may differ from the reference program's by a relative error of at most 0.0018.
Values may be sent and summed in bfloat16 or wider, within the bound.
A program may use at most 64 MiB of HBM per device.

```python
import math
import jax
import jax.numpy as jnp
from jax import lax

D_IN = 2560
KVH = 4
HEAD = 128
STEP = 8
TOK_DEV = 256
VW = 512
TOKENS_ALL = 8192
N_FSDP = 32
N_DP = 1


def strengthened(entries, rng, source, target, parts, factor):
    def block_of(axis_at):
        return (jnp.arange(entries.shape[axis_at]) // (entries.shape[axis_at] // parts)).reshape((-1,) + (1,) * (entries.ndim - 1 - axis_at))

    first = jax.random.permutation(rng, parts)[block_of(target)]
    far = (block_of(target) + parts // 2) % parts
    return jnp.where((block_of(source) == first) | (block_of(source) == far), factor * entries, entries)


def block_levels(stream_key, shape, cuts, smallest, largest):
    gain = 1.0
    for axis_at, blocks in cuts:
        heights = jax.random.uniform(jax.random.fold_in(jax.random.fold_in(stream_key, 6), axis_at), (blocks,), jnp.float32, smallest / len(cuts), largest / len(cuts))
        gain = gain * jnp.repeat(jnp.exp(heights), shape[axis_at] // blocks).reshape((-1,) + (1,) * (len(shape) - 1 - axis_at))
    return gain


def bell_draw(rng, extent, scale, limit, split=(), dtype=jnp.bfloat16):
    array = scale * jax.random.normal(rng, extent, jnp.float32)
    if split:
        array = array * block_levels(rng, extent, split, -0.22, 0.18)
    return jnp.clip(array, -limit, limit).astype(dtype)


def gaussian_with(key, shape, scale, limit, split, heavy, held_as=jnp.bfloat16):
    entries = scale * jax.random.normal(key, shape, jnp.float32)
    if split:
        entries = entries * block_levels(key, shape, split, -0.22, 0.18)
    return jnp.clip(strengthened(entries, jax.random.fold_in(key, 3), *heavy), -limit, limit).astype(held_as)


def setup_inputs(seed: int = 0) -> dict:
    splits = jax.random.split(jax.random.key(seed), 6)
    return {
        "inputs": gaussian_with(splits[0], (TOKENS_ALL, D_IN), 1.0, 6.0, ((0, 32),), (0, 1, 32, 2.75)),
        "value_cotangent": bell_draw(splits[1], (TOKENS_ALL, VW), ((TOK_DEV * N_FSDP * N_DP) ** -0.5), 0.15625, ((0, 32),)),
        "master": bell_draw(splits[2], (D_IN, KVH, HEAD), D_IN ** -0.5, 0.125, ((0, 32),), jnp.float32),
        "first_moment": bell_draw(splits[3], (D_IN, KVH, HEAD), 1.0, 6.0, ((0, 32),), jnp.float32),
        "second_moment": jnp.clip(jnp.exp(math.log(4.0) - 2.7725887 * jax.random.uniform(splits[4], (D_IN, KVH, HEAD), jnp.float32) ** block_levels(splits[4], (D_IN, KVH, HEAD), ((0, 32),), -0.2, 0.2)), 0.25, 4.0),
    }


beta_first = 0.9
beta_second = 0.95
learn_rate = 0.001
weight_decay = 0.1
epsilon = 1e-08

def reference(inputs, value_cotangent, master, first_moment, second_moment):
    gradient = lax.dot_general(inputs, value_cotangent, (((0,), (0,)), ((), ())), preferred_element_type=jnp.float32)
    gradient = gradient.reshape(D_IN, KVH, HEAD)
    moment_one_new = beta_first * first_moment + (1.0 - beta_first) * gradient
    moment_two_new = beta_second * second_moment + (1.0 - beta_second) * gradient * gradient
    correct_one = 1.0 - beta_first ** STEP
    correct_two = 1.0 - beta_second ** STEP
    update = moment_one_new / correct_one / (jnp.sqrt(moment_two_new / correct_two) + epsilon) + weight_decay * master
    master_new = master - learn_rate * update
    narrow_weight = master_new.astype(jnp.bfloat16)
    head_order = (jnp.arange(N_FSDP) % KVH).astype(jnp.int32)
    picked = jnp.take(narrow_weight, head_order, axis=1)
    head_blocks = jnp.transpose(picked, (1, 0, 2))
    return (moment_one_new, moment_two_new, master_new, head_blocks)
```

```python
import functools

import jax
import jax.numpy as jnp
from jax import lax
from jax.experimental import pallas as pl
from jax.experimental.pallas import tpu as pltpu
from jax.sharding import PartitionSpec as P

STEP = 8


beta_first = 0.9
beta_second = 0.95
learn_rate = 0.001
weight_decay = 0.1
epsilon = 1e-08


def adam_update(gradient, moment_one, moment_two, weights):
    moment_one_new = beta_first * moment_one + (1.0 - beta_first) * gradient
    moment_two_new = beta_second * moment_two + (1.0 - beta_second) * gradient * gradient
    correct_one = 1.0 - beta_first**STEP
    correct_two = 1.0 - beta_second**STEP
    update = (
        moment_one_new / correct_one / (jnp.sqrt(moment_two_new / correct_two) + epsilon)
        + weight_decay * weights
    )
    return (moment_one_new, moment_two_new, weights - learn_rate * update)


def shards(inputs, value_cotangent, master, first_moment, second_moment):
    _, heads, slice_width = master.shape
    head_size = value_cotangent.shape[1] // heads
    head_parts = []
    for head in range(heads):
        head_cot = value_cotangent[:, head * head_size : (head + 1) * head_size]
        head_term = lax.dot_general(
            inputs, head_cot, (((0,), (0,)), ((), ())), preferred_element_type=jnp.float32
        )
        head_parts.append(
            lax.psum_scatter(
                head_term.astype(jnp.bfloat16), "dp", scatter_dimension=1, tiled=True
            ).astype(jnp.float32)
        )
    column_part = jnp.stack(head_parts, axis=1)
    grad_share = lax.psum_scatter(column_part, "fsdp", scatter_dimension=0, tiled=True)
    moment_one_new, moment_two_new, master_new = adam_update(
        grad_share, first_moment, second_moment, master
    )
    narrow_weight = master_new.astype(jnp.bfloat16)
    gathered = lax.all_gather(narrow_weight, "fsdp", axis=0, tiled=True)
    head_index = lax.axis_index("fsdp") % heads
    picked = lax.dynamic_slice_in_dim(gathered, head_index, 1, 1)
    tp_block = picked.reshape(1, gathered.shape[0], slice_width)
    return (moment_one_new, moment_two_new, master_new, tp_block)


def step_kernel(
    n, x_ref, g_ref, w_ref, m_ref, v_ref, m_out, v_out, w_out, tp_out,
    mate_x, mate_g, total, parts, arrived, narrow,
    mate_send, mate_recv, part_send, part_recv, row_send, row_recv,
):
    me = lax.axis_index("fsdp")
    core = lax.rem(me, 2)
    chip = me // 2
    mate = me + 1 - 2 * core
    chips = n // 2
    rows, heads, head_size = w_ref.shape
    half = x_ref.shape[1] // 2

    barrier = pltpu.get_barrier_semaphore()
    for step in range(1, n):
        pl.semaphore_signal(
            barrier, inc=1, device_id={"fsdp": lax.rem(me + step, n)},
            device_id_type=pl.DeviceIdType.MESH,
        )
    pl.semaphore_wait(barrier, n - 1)

    def columns(owner):
        return pl.ds(pl.multiple_of(owner * half, 128), half)

    swap_x = pltpu.make_async_remote_copy(
        x_ref.at[:, columns(1 - core)], mate_x, mate_send.at[0], mate_recv.at[0],
        device_id={"fsdp": mate}, device_id_type=pl.DeviceIdType.MESH,
    )
    swap_g = pltpu.make_async_remote_copy(
        g_ref, mate_g, mate_send.at[1], mate_recv.at[1],
        device_id={"fsdp": mate}, device_id_type=pl.DeviceIdType.MESH,
    )
    swap_g.start()
    swap_x.start()

    def transposed_dot(left, right):
        return lax.dot_general(
            left, right, (((0,), (0,)), ((), ())), preferred_element_type=jnp.float32
        )

    tiles = 2
    tile = half // tiles
    per_tile = chips // tiles
    for t in range(tiles):
        own = x_ref[:, pl.ds(pl.multiple_of(core * half + t * tile, 128), tile)]
        total[t * tile : (t + 1) * tile, :] = transposed_dot(own, g_ref[...])
    swap_g.wait_recv()
    swap_x.wait_recv()

    def part_copy(slot):
        return pltpu.make_async_remote_copy(
            parts.at[pl.ds(pl.multiple_of(slot * rows, 16), rows)],
            arrived.at[chip],
            part_send.at[slot],
            part_recv.at[chip],
            device_id={"fsdp": core * chips + slot},
            device_id_type=pl.DeviceIdType.MESH,
        )

    for t in range(tiles):
        block = slice(t * tile, (t + 1) * tile)
        parts[block, :] = (
            total[block, :] + transposed_dot(mate_x[:, block], mate_g[...])
        ).astype(jnp.bfloat16)
        for step in range(per_tile):
            slot = t * per_tile + lax.rem(chip + step, per_tile)

            @pl.when(core * chips + slot != me)
            def _():
                part_copy(slot).start()

    worker = me // chips
    own_slot = lax.rem(me, chips)

    @pl.when(worker == core)
    def _():
        arrived[chip] = parts[pl.ds(pl.multiple_of(own_slot * rows, 16), rows), :]

    def wait_part(source):
        pltpu.make_async_remote_copy(
            parts.at[pl.ds(0, rows)], arrived.at[source], part_send.at[0],
            part_recv.at[source], device_id={"fsdp": mate},
            device_id_type=pl.DeviceIdType.MESH,
        ).wait_recv()

    for source in range(chips):
        @pl.when(2 * source + worker != me)
        def _():
            wait_part(source)

    for head in range(heads):
        span = slice(head * head_size, (head + 1) * head_size)
        gradient = arrived[0, :, span].astype(jnp.float32)
        for source in range(1, chips):
            gradient = gradient + arrived[source, :, span].astype(jnp.float32)
        m_new, v_new, w_new = adam_update(
            gradient, m_ref[:, head, :], v_ref[:, head, :], w_ref[:, head, :]
        )
        m_out[:, head, :] = m_new
        v_out[:, head, :] = v_new
        w_out[:, head, :] = w_new
        narrow[head] = w_new.astype(jnp.bfloat16)

    def own_rows(owner):
        return pl.ds(pl.multiple_of(owner * rows, 16), rows)

    def row_copy(target):
        return pltpu.make_async_remote_copy(
            narrow.at[lax.rem(target, heads)],
            tp_out.at[0, own_rows(me)],
            row_send.at[target],
            row_recv.at[me],
            device_id={"fsdp": target},
            device_id_type=pl.DeviceIdType.MESH,
        )

    for step in range(1, n):
        row_copy(lax.rem(me + step, n)).start()
    tp_out[0, own_rows(me), :] = narrow[lax.rem(me, heads)]

    swap_g.wait_send()
    swap_x.wait_send()
    for slot in range(chips):
        @pl.when(core * chips + slot != me)
        def _():
            part_copy(slot).wait_send()
    for step in range(1, n):
        other = lax.rem(me + step, n)
        row_copy(other).wait_send()
        pltpu.make_async_remote_copy(
            narrow.at[0], tp_out.at[0, own_rows(other)], row_send.at[other],
            row_recv.at[other], device_id={"fsdp": other},
            device_id_type=pl.DeviceIdType.MESH,
        ).wait_recv()


def fused(n, inputs, value_cotangent, master, first_moment, second_moment):
    tokens, features = inputs.shape
    width = value_cotangent.shape[1]
    rows, heads, head_size = master.shape
    chips = n // 2
    state = jax.ShapeDtypeStruct(master.shape, jnp.float32)
    vmem = pl.BlockSpec(memory_space=pltpu.VMEM)
    return pl.pallas_call(
        functools.partial(step_kernel, n),
        out_shape=(
            state, state, state,
            jax.ShapeDtypeStruct((1, features, head_size), jnp.bfloat16),
        ),
        in_specs=[vmem] * 5,
        out_specs=[vmem] * 4,
        scratch_shapes=[
            pltpu.VMEM((tokens, features // 2), jnp.bfloat16),
            pltpu.VMEM((tokens, width), jnp.bfloat16),
            pltpu.VMEM((features // 2, width), jnp.float32),
            pltpu.VMEM((features // 2, width), jnp.bfloat16),
            pltpu.VMEM((chips, rows, width), jnp.bfloat16),
            pltpu.VMEM((heads, rows, head_size), jnp.bfloat16),
            pltpu.SemaphoreType.DMA((2,)),
            pltpu.SemaphoreType.DMA((2,)),
            pltpu.SemaphoreType.DMA((chips,)),
            pltpu.SemaphoreType.DMA((chips,)),
            pltpu.SemaphoreType.DMA((n,)),
            pltpu.SemaphoreType.DMA((n,)),
        ],
        compiler_params=pltpu.CompilerParams(collective_id=0, has_side_effects=True),
    )(inputs, value_cotangent, master, first_moment, second_moment)


def solution(mesh):
    n = mesh.shape["fsdp"]

    def body(inputs, value_cotangent, master, first_moment, second_moment):
        rows = master.shape[0]
        direct = (
            mesh.shape["dp"] == 1
            and n % 4 == 0
            and inputs.shape[1] % 512 == 0
            and rows % 16 == 0
            and master.shape[2] % 128 == 0
        )
        if direct:
            return fused(n, inputs, value_cotangent, master, first_moment, second_moment)
        return shards(inputs, value_cotangent, master, first_moment, second_moment)

    placed = (
        P(("fsdp", "dp"), None),
        P(("fsdp", "dp"), None),
        P("fsdp", None, "dp"),
        P("fsdp", None, "dp"),
        P("fsdp", None, "dp"),
    )
    return jax.shard_map(
        body,
        mesh=mesh,
        in_specs=placed,
        out_specs=(
            P("fsdp", None, "dp"),
            P("fsdp", None, "dp"),
            P("fsdp", None, "dp"),
            P("fsdp", None, "dp"),
        ),
        check_vma=False,
    )
```

```python
import functools

import jax
import jax.numpy as jnp
from jax import lax
from jax.experimental import pallas as pl
from jax.experimental.pallas import tpu as pltpu
from jax.sharding import PartitionSpec as P

STEP = 8


beta_first = 0.9
beta_second = 0.95
learn_rate = 0.001
weight_decay = 0.1
epsilon = 1e-08


def adam_update(gradient, moment_one, moment_two, weights):
    moment_one_new = beta_first * moment_one + (1.0 - beta_first) * gradient
    moment_two_new = beta_second * moment_two + (1.0 - beta_second) * gradient * gradient
    correct_one = 1.0 - beta_first**STEP
    correct_two = 1.0 - beta_second**STEP
    update = (
        moment_one_new / correct_one / (jnp.sqrt(moment_two_new / correct_two) + epsilon)
        + weight_decay * weights
    )
    return (moment_one_new, moment_two_new, weights - learn_rate * update)


def shards(inputs, value_cotangent, master, first_moment, second_moment):
    _, heads, slice_width = master.shape
    head_size = value_cotangent.shape[1] // heads
    head_parts = []
    for head in range(heads):
        head_cot = value_cotangent[:, head * head_size : (head + 1) * head_size]
        head_term = lax.dot_general(
            inputs, head_cot, (((0,), (0,)), ((), ())), preferred_element_type=jnp.float32
        )
        head_parts.append(
            lax.psum_scatter(
                head_term.astype(jnp.bfloat16), "dp", scatter_dimension=1, tiled=True
            ).astype(jnp.float32)
        )
    column_part = jnp.stack(head_parts, axis=1)
    grad_share = lax.psum_scatter(column_part, "fsdp", scatter_dimension=0, tiled=True)
    moment_one_new, moment_two_new, master_new = adam_update(
        grad_share, first_moment, second_moment, master
    )
    narrow_weight = master_new.astype(jnp.bfloat16)
    gathered = lax.all_gather(narrow_weight, "fsdp", axis=0, tiled=True)
    head_index = lax.axis_index("fsdp") % heads
    picked = lax.dynamic_slice_in_dim(gathered, head_index, 1, 1)
    tp_block = picked.reshape(1, gathered.shape[0], slice_width)
    return (moment_one_new, moment_two_new, master_new, tp_block)


PLANE = 8


def head_of(slot, heads):
    return slot * 2 % heads + slot * 2 // heads


def step_kernel(
    n, x_hbm, g_hbm, w_hbm, m_hbm, v_hbm, grad_out, tp_out,
    x_ref, g_ref, w_ref, m_ref, v_ref,
    mate_x, mate_g, total, parts, plane_in, column_part, column_in, blocks,
    load_sem, mate_send, mate_recv, plane_send, plane_recv,
    column_send, column_recv, line_send, line_recv, row_send, row_recv,
):
    me = lax.axis_index("fsdp")
    z = me // PLANE
    q = lax.rem(me, PLANE)
    spot = q // 2
    core = lax.rem(q, 2)
    mate = me + 1 - 2 * core
    spots = PLANE // 2
    depth = n // PLANE
    layers = depth // 2
    rows, heads, head_size = w_ref.shape
    pair = heads // 2
    half = x_ref.shape[1] // 2
    tile = half // layers
    both = 2 * rows
    worker = z // layers

    loads = [
        pltpu.make_async_copy(source, target, load_sem.at[i])
        for i, (source, target) in enumerate(
            ((g_hbm, g_ref), (x_hbm, x_ref), (w_hbm, w_ref), (m_hbm, m_ref), (v_hbm, v_ref))
        )
    ]
    for load in loads:
        load.start()

    def to(device):
        return dict(device_id={"fsdp": device}, device_id_type=pl.DeviceIdType.MESH)

    def plane_mate(step):
        return z * PLANE + lax.rem(q + step, PLANE)

    def layer(step):
        return lax.rem(z + step, depth)

    barrier = pltpu.get_barrier_semaphore()
    for step in range(1, PLANE):
        pl.semaphore_signal(barrier, inc=1, **to(plane_mate(step)))
    for step in range(1, depth):
        for side in range(2):
            pl.semaphore_signal(
                barrier, inc=1, **to(layer(step) * PLANE + 2 * spot + side)
            )
    loads[0].wait()
    loads[1].wait()
    pl.semaphore_wait(barrier, PLANE - 1 + 2 * (depth - 1))

    swap_g = pltpu.make_async_remote_copy(
        g_ref, mate_g, mate_send.at[0], mate_recv.at[0], **to(mate)
    )
    swap_x = pltpu.make_async_remote_copy(
        x_ref.at[:, pl.ds(pl.multiple_of((1 - core) * half, 128), half)],
        mate_x, mate_send.at[1], mate_recv.at[1], **to(mate)
    )
    swap_g.start()
    swap_x.start()

    def transposed_dot(left, right):
        return lax.dot_general(
            left, right, (((0,), (0,)), ((), ())), preferred_element_type=jnp.float32
        )

    def columns_of(ref, phase):
        return jnp.concatenate(
            [
                ref[:, head_of(s, heads) * head_size : (head_of(s, heads) + 1) * head_size]
                for s in range(phase * pair, (phase + 1) * pair)
            ],
            axis=1,
        )

    wide = pair * head_size
    for phase in range(2):
        right = columns_of(g_ref, phase)
        for t in range(layers):
            own = x_ref[:, pl.ds(pl.multiple_of(core * half + t * tile, 128), tile)]
            total[t * tile : (t + 1) * tile, phase * wide : (phase + 1) * wide] = (
                transposed_dot(own, right)
            )
    swap_g.wait_recv()
    swap_x.wait_recv()

    def of_phase(phase):
        return pl.ds(phase * pair, pair)

    def plane_copy(phase, t, step, source):
        index = (phase * layers + t) * spots
        target = lax.rem(spot + step, spots)
        return pltpu.make_async_remote_copy(
            parts.at[
                of_phase(phase), pl.ds(pl.multiple_of(t * tile + target * both, 16), both)
            ],
            plane_in.at[source, of_phase(phase), pl.ds(t * both, both)],
            plane_send.at[index + target],
            plane_recv.at[index + source],
            **to(z * PLANE + 2 * target + core),
        )

    for phase in range(2):
        right = columns_of(mate_g, phase)
        for t in range(layers):
            block = slice(t * tile, (t + 1) * tile)
            summed = (
                total[block, phase * wide : (phase + 1) * wide]
                + transposed_dot(mate_x[:, block], right)
            ).astype(jnp.bfloat16)
            for j in range(pair):
                parts[phase * pair + j, block, :] = summed[
                    :, j * head_size : (j + 1) * head_size
                ]
            for step in range(1, spots):
                plane_copy(phase, t, step, spot).start()

    def column_copy(phase, t, side, source):
        index = (phase * layers + t) * 2 + side
        return pltpu.make_async_remote_copy(
            column_part.at[of_phase(phase), pl.ds(t * both + side * rows, rows)],
            column_in.at[source, of_phase(phase)],
            column_send.at[index],
            column_recv.at[phase * depth + source],
            **to((core * layers + t) * PLANE + 2 * spot + side),
        )

    def is_me(t, side):
        return (core * layers + t) * PLANE + 2 * spot + side == me

    def plane_sum(phase, t):
        for step in range(1, spots):
            plane_copy(phase, t, step, lax.rem(spot + step, spots)).wait_recv()
        span = slice(phase * pair, (phase + 1) * pair)
        value = parts[
            span, pl.ds(pl.multiple_of(t * tile + spot * both, 16), both), :
        ].astype(jnp.float32)
        for step in range(1, spots):
            value = value + plane_in[
                lax.rem(spot + step, spots), span, t * both : (t + 1) * both, :
            ].astype(jnp.float32)
        column_part[span, t * both : (t + 1) * both, :] = value.astype(jnp.bfloat16)
        for side in range(2):
            @pl.when(jnp.logical_not(is_me(t, side)))
            def _():
                column_copy(phase, t, side, z).start()

            @pl.when(is_me(t, side))
            def _():
                column_in[z, span] = column_part[
                    span, t * both + side * rows : t * both + (side + 1) * rows, :
                ]

    def line_copy(phase, step, source):
        target = layer(step)
        return pltpu.make_async_remote_copy(
            blocks.at[z, of_phase(phase)],
            blocks.at[source, of_phase(phase)],
            line_send.at[phase * depth + target],
            line_recv.at[phase * depth + source],
            **to(target * PLANE + q),
        )

    def rows_of(owner):
        return pl.ds(pl.multiple_of(owner * rows, 16), rows)

    def slot_of(device):
        head = lax.rem(device, heads)
        return lax.rem(head, 2) * pair + head // 2

    def row_copy(source, target):
        return pltpu.make_async_remote_copy(
            blocks.at[source, slot_of(target)],
            tp_out.at[0, rows_of(source * PLANE + q)],
            row_send.at[source * PLANE + target],
            row_recv.at[source * PLANE + q],
            **to(z * PLANE + target),
        )

    def spread(phase, source):
        for step in range(1, spots):
            row_copy(source, 2 * lax.rem(spot + step, spots) + phase).start()

        @pl.when(core != phase)
        def _():
            row_copy(source, 2 * spot + phase).start()

        @pl.when(core == phase)
        def _():
            tp_out[0, rows_of(source * PLANE + q), :] = blocks[source, slot_of(me)]

    def update(phase):
        for source in range(depth):
            @pl.when(source * PLANE + 2 * spot + worker != me)
            def _():
                column_copy(phase, 0, 0, source).wait_recv()
        for s in range(phase * pair, (phase + 1) * pair):
            head = head_of(s, heads)
            gradient = column_in[0, s].astype(jnp.float32)
            for source in range(1, depth):
                gradient = gradient + column_in[source, s].astype(jnp.float32)
            grad_out[s] = gradient
            _, _, w_new = adam_update(
                gradient, m_ref[:, head, :], v_ref[:, head, :], w_ref[:, head, :]
            )
            blocks[z, s] = w_new.astype(jnp.bfloat16)
        for step in range(depth - 1, 0, -1):
            line_copy(phase, step, z).start()
        spread(phase, z)

    def forward(phase):
        for step in range(1, depth):
            source = layer(step)
            line_copy(phase, step, source).wait_recv()
            spread(phase, source)

    pieces = [(phase, t) for phase in range(2) for t in range(layers)]
    for piece in pieces[: layers + 1]:
        plane_sum(*piece)
    for load in loads[2:]:
        load.wait()
    update(0)
    for piece in pieces[layers + 1 :]:
        plane_sum(*piece)
    forward(0)
    update(1)
    forward(1)

    swap_g.wait_send()
    swap_x.wait_send()
    for phase, t in pieces:
        for step in range(1, spots):
            plane_copy(phase, t, step, spot).wait_send()
        for side in range(2):
            @pl.when(jnp.logical_not(is_me(t, side)))
            def _():
                column_copy(phase, t, side, z).wait_send()
    for phase in range(2):
        for step in range(1, depth):
            line_copy(phase, step, z).wait_send()
    for source in range(depth):
        for step in range(1, PLANE):
            other = lax.rem(q + step, PLANE)
            row_copy(source, other).wait_send()
            pltpu.make_async_remote_copy(
                blocks.at[0, 0], tp_out.at[0, rows_of(source * PLANE + other)],
                row_send.at[0], row_recv.at[source * PLANE + other], **to(mate),
            ).wait_recv()


def finish_kernel(g_ref, tp_ref, w_ref, m_ref, v_ref, m_out, v_out, w_out, tp_out):
    heads = g_ref.shape[0]
    for s in range(heads):
        head = head_of(s, heads)
        m_new, v_new, w_new = adam_update(
            g_ref[s], m_ref[:, head, :], v_ref[:, head, :], w_ref[:, head, :]
        )
        m_out[:, head, :] = m_new
        v_out[:, head, :] = v_new
        w_out[:, head, :] = w_new
    tp_out[...] = tp_ref[...]


def fused(n, inputs, value_cotangent, master, first_moment, second_moment):
    tokens, features = inputs.shape
    width = value_cotangent.shape[1]
    rows, heads, head_size = master.shape
    half = features // 2
    depth = n // PLANE
    layers = depth // 2
    spots = PLANE // 2
    state = jax.ShapeDtypeStruct(master.shape, jnp.float32)
    block = jax.ShapeDtypeStruct((1, features, head_size), jnp.bfloat16)
    vmem = pl.BlockSpec(memory_space=pltpu.VMEM)
    narrow = jnp.bfloat16
    gradient, gathered = pl.pallas_call(
        functools.partial(step_kernel, n),
        out_shape=(jax.ShapeDtypeStruct((heads, rows, head_size), jnp.float32), block),
        in_specs=[pl.BlockSpec(memory_space=pl.ANY)] * 5,
        out_specs=[vmem] * 2,
        scratch_shapes=[
            pltpu.VMEM((tokens, features), narrow),
            pltpu.VMEM((tokens, width), narrow),
            pltpu.VMEM(master.shape, jnp.float32),
            pltpu.VMEM(master.shape, jnp.float32),
            pltpu.VMEM(master.shape, jnp.float32),
            pltpu.VMEM((tokens, half), narrow),
            pltpu.VMEM((tokens, width), narrow),
            pltpu.VMEM((half, width), jnp.float32),
            pltpu.VMEM((heads, half, head_size), narrow),
            pltpu.VMEM((spots, heads, layers * 2 * rows, head_size), narrow),
            pltpu.VMEM((heads, layers * 2 * rows, head_size), narrow),
            pltpu.VMEM((depth, heads, rows, head_size), narrow),
            pltpu.VMEM((depth, heads, rows, head_size), narrow),
            pltpu.SemaphoreType.DMA((5,)),
            pltpu.SemaphoreType.DMA((2,)),
            pltpu.SemaphoreType.DMA((2,)),
            pltpu.SemaphoreType.DMA((2 * layers * spots,)),
            pltpu.SemaphoreType.DMA((2 * layers * spots,)),
            pltpu.SemaphoreType.DMA((2 * layers * 2,)),
            pltpu.SemaphoreType.DMA((2 * depth,)),
            pltpu.SemaphoreType.DMA((2 * depth,)),
            pltpu.SemaphoreType.DMA((2 * depth,)),
            pltpu.SemaphoreType.DMA((n,)),
            pltpu.SemaphoreType.DMA((n,)),
        ],
        compiler_params=pltpu.CompilerParams(collective_id=0, has_side_effects=True),
    )(inputs, value_cotangent, master, first_moment, second_moment)
    return pl.pallas_call(
        finish_kernel,
        out_shape=(state, state, state, block),
        in_specs=[vmem] * 5,
        out_specs=[vmem] * 4,
    )(gradient, gathered, master, first_moment, second_moment)


def solution(mesh):
    n = mesh.shape["fsdp"]

    def body(inputs, value_cotangent, master, first_moment, second_moment):
        rows = master.shape[0]
        direct = (
            mesh.shape["dp"] == 1
            and n % (2 * PLANE) == 0
            and inputs.shape[1] % (256 * (n // (2 * PLANE))) == 0
            and rows % 16 == 0
            and master.shape[1] % 2 == 0
            and PLANE % master.shape[1] == 0
            and master.shape[2] % 128 == 0
        )
        if direct:
            return fused(n, inputs, value_cotangent, master, first_moment, second_moment)
        return shards(inputs, value_cotangent, master, first_moment, second_moment)

    placed = (
        P(("fsdp", "dp"), None),
        P(("fsdp", "dp"), None),
        P("fsdp", None, "dp"),
        P("fsdp", None, "dp"),
        P("fsdp", None, "dp"),
    )
    return jax.shard_map(
        body,
        mesh=mesh,
        in_specs=placed,
        out_specs=(
            P("fsdp", None, "dp"),
            P("fsdp", None, "dp"),
            P("fsdp", None, "dp"),
            P("fsdp", None, "dp"),
        ),
        check_vma=False,
    )
```

```python
import functools

import jax
import jax.numpy as jnp
from jax import lax
from jax.experimental import pallas as pl
from jax.experimental.pallas import tpu as pltpu
from jax.sharding import PartitionSpec as P

STEP = 8


beta_first = 0.9
beta_second = 0.95
learn_rate = 0.001
weight_decay = 0.1
epsilon = 1e-08


def adam_update(gradient, moment_one, moment_two, weights):
    moment_one_new = beta_first * moment_one + (1.0 - beta_first) * gradient
    moment_two_new = beta_second * moment_two + (1.0 - beta_second) * gradient * gradient
    correct_one = 1.0 - beta_first**STEP
    correct_two = 1.0 - beta_second**STEP
    update = (
        moment_one_new / correct_one / (jnp.sqrt(moment_two_new / correct_two) + epsilon)
        + weight_decay * weights
    )
    return (moment_one_new, moment_two_new, weights - learn_rate * update)


def shards(inputs, value_cotangent, master, first_moment, second_moment):
    _, heads, slice_width = master.shape
    head_size = value_cotangent.shape[1] // heads
    head_parts = []
    for head in range(heads):
        head_cot = value_cotangent[:, head * head_size : (head + 1) * head_size]
        head_term = lax.dot_general(
            inputs, head_cot, (((0,), (0,)), ((), ())), preferred_element_type=jnp.float32
        )
        head_parts.append(
            lax.psum_scatter(
                head_term.astype(jnp.bfloat16), "dp", scatter_dimension=1, tiled=True
            ).astype(jnp.float32)
        )
    column_part = jnp.stack(head_parts, axis=1)
    grad_share = lax.psum_scatter(column_part, "fsdp", scatter_dimension=0, tiled=True)
    moment_one_new, moment_two_new, master_new = adam_update(
        grad_share, first_moment, second_moment, master
    )
    narrow_weight = master_new.astype(jnp.bfloat16)
    gathered = lax.all_gather(narrow_weight, "fsdp", axis=0, tiled=True)
    head_index = lax.axis_index("fsdp") % heads
    picked = lax.dynamic_slice_in_dim(gathered, head_index, 1, 1)
    tp_block = picked.reshape(1, gathered.shape[0], slice_width)
    return (moment_one_new, moment_two_new, master_new, tp_block)


VMEM_BYTES = 67043328
SPARE_BYTES = 64 * 1024
PLANE = 8


def step_kernel(
    n, x_hbm, g_hbm, w_hbm, m_hbm, v_hbm, m_out, v_out, w_out, tp_out,
    x_ref, g_ref, w_ref, m_ref, v_ref,
    mate_x, mate_g, total, parts, plane_in, column_part, column_in, blocks,
    load_sem, mate_send, mate_recv, plane_send, plane_recv,
    column_send, column_recv, line_send, line_recv, row_send, row_recv,
):
    me = lax.axis_index("fsdp")
    z = me // PLANE
    q = lax.rem(me, PLANE)
    spot = q // 2
    core = lax.rem(q, 2)
    mate = me + 1 - 2 * core
    spots = PLANE // 2
    depth = n // PLANE
    layers = depth // 2
    rows, heads, head_size = w_ref.shape
    half = x_ref.shape[1] // 2
    tile = half // layers
    both = 2 * rows
    worker = z // layers

    loads = [
        pltpu.make_async_copy(source, target, load_sem.at[i])
        for i, (source, target) in enumerate(
            ((g_hbm, g_ref), (x_hbm, x_ref), (w_hbm, w_ref), (m_hbm, m_ref), (v_hbm, v_ref))
        )
    ]
    for load in loads:
        load.start()

    def to(device):
        return dict(device_id={"fsdp": device}, device_id_type=pl.DeviceIdType.MESH)

    def plane_mate(step):
        return z * PLANE + lax.rem(q + step, PLANE)

    def layer(step):
        return lax.rem(z + step, depth)

    barrier = pltpu.get_barrier_semaphore()
    for step in range(1, PLANE):
        pl.semaphore_signal(barrier, inc=1, **to(plane_mate(step)))
    for step in range(1, depth):
        for side in range(2):
            pl.semaphore_signal(
                barrier, inc=1, **to(layer(step) * PLANE + 2 * spot + side)
            )
    loads[0].wait()
    loads[1].wait()
    pl.semaphore_wait(barrier, PLANE - 1 + 2 * (depth - 1))

    swap_g = pltpu.make_async_remote_copy(
        g_ref, mate_g, mate_send.at[0], mate_recv.at[0], **to(mate)
    )
    swap_x = pltpu.make_async_remote_copy(
        x_ref.at[:, pl.ds(pl.multiple_of((1 - core) * half, 128), half)],
        mate_x, mate_send.at[1], mate_recv.at[1], **to(mate)
    )
    swap_g.start()
    swap_x.start()

    def transposed_dot(left, right):
        return lax.dot_general(
            left, right, (((0,), (0,)), ((), ())), preferred_element_type=jnp.float32
        )

    def rows_of_tile(t):
        return slice(t * tile, (t + 1) * tile)

    for t in range(layers):
        own = x_ref[:, pl.ds(pl.multiple_of(core * half + t * tile, 128), tile)]
        total[rows_of_tile(t), :] = transposed_dot(own, g_ref[...])
    swap_g.wait_recv()
    swap_x.wait_recv()

    def plane_copy(phase, t, step, source):
        index = (phase * layers + t) * spots
        target = lax.rem(spot + step, spots)
        return pltpu.make_async_remote_copy(
            parts.at[
                phase, pl.ds(pl.multiple_of(t * tile + target * both, 16), both)
            ],
            plane_in.at[source, phase, pl.ds(t * both, both)],
            plane_send.at[index + target],
            plane_recv.at[index + source],
            **to(z * PLANE + 2 * target + core),
        )

    for t in range(layers):
        block = rows_of_tile(t)
        summed = (
            total[block, :] + transposed_dot(mate_x[:, block], mate_g[...])
        ).astype(jnp.bfloat16)
        for head in range(heads):
            parts[head, block, :] = summed[:, head * head_size : (head + 1) * head_size]
        for step in range(1, spots):
            plane_copy(0, t, step, spot).start()
    for phase in range(1, heads):
        for t in range(layers):
            for step in range(1, spots):
                plane_copy(phase, t, step, spot).start()

    def column_copy(phase, t, side, source):
        index = (phase * layers + t) * 2 + side
        return pltpu.make_async_remote_copy(
            column_part.at[phase, pl.ds(t * both + side * rows, rows)],
            column_in.at[source, phase],
            column_send.at[index],
            column_recv.at[phase * depth + source],
            **to((core * layers + t) * PLANE + 2 * spot + side),
        )

    def is_me(t, side):
        return (core * layers + t) * PLANE + 2 * spot + side == me

    def plane_sum(phase, t):
        for step in range(1, spots):
            plane_copy(phase, t, step, lax.rem(spot + step, spots)).wait_recv()
        value = parts[
            phase, pl.ds(pl.multiple_of(t * tile + spot * both, 16), both), :
        ].astype(jnp.float32)
        for step in range(1, spots):
            value = value + plane_in[
                lax.rem(spot + step, spots), phase, t * both : (t + 1) * both, :
            ].astype(jnp.float32)
        column_part[phase, t * both : (t + 1) * both, :] = value.astype(jnp.bfloat16)
        for side in range(2):
            @pl.when(jnp.logical_not(is_me(t, side)))
            def _():
                column_copy(phase, t, side, z).start()

            @pl.when(is_me(t, side))
            def _():
                column_in[z, phase] = column_part[
                    phase, t * both + side * rows : t * both + (side + 1) * rows, :
                ]

    def line_copy(phase, step, source):
        target = layer(step)
        return pltpu.make_async_remote_copy(
            blocks.at[z, phase],
            blocks.at[source, phase],
            line_send.at[phase * depth + target],
            line_recv.at[phase * depth + source],
            **to(target * PLANE + q),
        )

    def rows_of(owner):
        return pl.ds(pl.multiple_of(owner * rows, 16), rows)

    def row_copy(source, target):
        return pltpu.make_async_remote_copy(
            blocks.at[source, lax.rem(target, heads)],
            tp_out.at[0, rows_of(source * PLANE + q)],
            row_send.at[source * PLANE + target],
            row_recv.at[source * PLANE + q],
            **to(z * PLANE + target),
        )

    def spread(phase, source):
        for target in range(phase, PLANE, heads):
            @pl.when(target != q)
            def _():
                row_copy(source, target).start()

            @pl.when(target == q)
            def _():
                tp_out[0, rows_of(source * PLANE + q), :] = blocks[source, phase]

    def update(phase):
        for source in range(depth):
            @pl.when(source * PLANE + 2 * spot + worker != me)
            def _():
                column_copy(phase, 0, 0, source).wait_recv()
        gradient = column_in[0, phase].astype(jnp.float32)
        for source in range(1, depth):
            gradient = gradient + column_in[source, phase].astype(jnp.float32)
        m_new, v_new, w_new = adam_update(
            gradient, m_ref[:, phase, :], v_ref[:, phase, :], w_ref[:, phase, :]
        )
        blocks[z, phase] = w_new.astype(jnp.bfloat16)
        for step in range(depth - 1, 0, -1):
            line_copy(phase, step, z).start()
        spread(phase, z)
        m_out[:, phase, :] = m_new
        v_out[:, phase, :] = v_new
        w_out[:, phase, :] = w_new

    def forward(phase):
        for step in range(1, depth):
            source = layer(step)
            line_copy(phase, step, source).wait_recv()
            spread(phase, source)

    pieces = [(phase, t) for phase in range(heads) for t in range(layers)]
    for phase in range(heads + 2):
        if phase < heads:
            for t in range(layers):
                plane_sum(phase, t)
        if phase == 1:
            for load in loads[2:]:
                load.wait()
        if 0 <= phase - 1 < heads:
            update(phase - 1)
        if 0 <= phase - 2 < heads:
            forward(phase - 2)

    swap_g.wait_send()
    swap_x.wait_send()
    for phase, t in pieces:
        for step in range(1, spots):
            plane_copy(phase, t, step, spot).wait_send()
        for side in range(2):
            @pl.when(jnp.logical_not(is_me(t, side)))
            def _():
                column_copy(phase, t, side, z).wait_send()
    for phase in range(heads):
        for step in range(1, depth):
            line_copy(phase, step, z).wait_send()
    for source in range(depth):
        for step in range(1, PLANE):
            other = lax.rem(q + step, PLANE)
            row_copy(source, other).wait_send()
            pltpu.make_async_remote_copy(
                blocks.at[0, 0], tp_out.at[0, rows_of(source * PLANE + other)],
                row_send.at[0], row_recv.at[source * PLANE + other], **to(mate),
            ).wait_recv()


def finish_kernel(*refs):
    count = (len(refs) - 1) // 2
    copies = [
        pltpu.make_async_copy(refs[i], refs[count + i], refs[-1].at[i])
        for i in range(count)
    ]
    for copy in copies:
        copy.start()
    for copy in copies:
        copy.wait()


def fused(n, inputs, value_cotangent, master, first_moment, second_moment):
    tokens, features = inputs.shape
    width = value_cotangent.shape[1]
    rows, heads, head_size = master.shape
    half = features // 2
    depth = n // PLANE
    layers = depth // 2
    spots = PLANE // 2
    state = jax.ShapeDtypeStruct(master.shape, jnp.float32)
    block = jax.ShapeDtypeStruct((1, features, head_size), jnp.bfloat16)
    results = 12 * master.size + 2 * block.size + SPARE_BYTES
    vmem = pl.BlockSpec(memory_space=pltpu.VMEM)
    narrow = jnp.bfloat16
    held = pl.pallas_call(
        functools.partial(step_kernel, n),
        out_shape=tuple(pltpu.VMEM(a.shape, a.dtype) for a in (state, state, state, block)),
        in_specs=[pl.BlockSpec(memory_space=pltpu.HBM)] * 5,
        out_specs=[vmem] * 4,
        scratch_shapes=[
            pltpu.VMEM((tokens, features), narrow),
            pltpu.VMEM((tokens, width), narrow),
            pltpu.VMEM(master.shape, jnp.float32),
            pltpu.VMEM(master.shape, jnp.float32),
            pltpu.VMEM(master.shape, jnp.float32),
            pltpu.VMEM((tokens, half), narrow),
            pltpu.VMEM((tokens, width), narrow),
            pltpu.VMEM((half, width), jnp.float32),
            pltpu.VMEM((heads, half, head_size), narrow),
            pltpu.VMEM((spots, heads, layers * 2 * rows, head_size), narrow),
            pltpu.VMEM((heads, layers * 2 * rows, head_size), narrow),
            pltpu.VMEM((depth, heads, rows, head_size), narrow),
            pltpu.VMEM((depth, heads, rows, head_size), narrow),
            pltpu.SemaphoreType.DMA((5,)),
            pltpu.SemaphoreType.DMA((2,)),
            pltpu.SemaphoreType.DMA((2,)),
            pltpu.SemaphoreType.DMA((heads * layers * spots,)),
            pltpu.SemaphoreType.DMA((heads * layers * spots,)),
            pltpu.SemaphoreType.DMA((heads * layers * 2,)),
            pltpu.SemaphoreType.DMA((heads * depth,)),
            pltpu.SemaphoreType.DMA((heads * depth,)),
            pltpu.SemaphoreType.DMA((heads * depth,)),
            pltpu.SemaphoreType.DMA((n,)),
            pltpu.SemaphoreType.DMA((n,)),
        ],
        compiler_params=pltpu.CompilerParams(
            collective_id=0, has_side_effects=True, vmem_limit_bytes=VMEM_BYTES - results
        ),
    )(inputs, value_cotangent, master, first_moment, second_moment)
    return pl.pallas_call(
        finish_kernel,
        out_shape=(state, state, state, block),
        in_specs=[vmem] * 4,
        out_specs=[pl.BlockSpec(memory_space=pltpu.HBM)] * 4,
        scratch_shapes=[pltpu.SemaphoreType.DMA((4,))],
        compiler_params=pltpu.CompilerParams(vmem_limit_bytes=VMEM_BYTES // 2),
    )(*held)


def solution(mesh):
    n = mesh.shape["fsdp"]

    def body(inputs, value_cotangent, master, first_moment, second_moment):
        rows = master.shape[0]
        direct = (
            mesh.shape["dp"] == 1
            and n % (2 * PLANE) == 0
            and inputs.shape[1] % (256 * (n // (2 * PLANE))) == 0
            and rows % 16 == 0
            and PLANE % master.shape[1] == 0
            and master.shape[2] % 128 == 0
        )
        if direct:
            return fused(n, inputs, value_cotangent, master, first_moment, second_moment)
        return shards(inputs, value_cotangent, master, first_moment, second_moment)

    placed = (
        P(("fsdp", "dp"), None),
        P(("fsdp", "dp"), None),
        P("fsdp", None, "dp"),
        P("fsdp", None, "dp"),
        P("fsdp", None, "dp"),
    )
    return jax.shard_map(
        body,
        mesh=mesh,
        in_specs=placed,
        out_specs=(
            P("fsdp", None, "dp"),
            P("fsdp", None, "dp"),
            P("fsdp", None, "dp"),
            P("fsdp", None, "dp"),
        ),
        check_vma=False,
    )
```

```python
import functools

import jax
import jax.numpy as jnp
from jax import lax
from jax.experimental import pallas as pl
from jax.experimental.pallas import tpu as pltpu
from jax.sharding import PartitionSpec as P

STEP = 8


beta_first = 0.9
beta_second = 0.95
learn_rate = 0.001
weight_decay = 0.1
epsilon = 1e-08


def adam_update(gradient, moment_one, moment_two, weights):
    moment_one_new = beta_first * moment_one + (1.0 - beta_first) * gradient
    moment_two_new = beta_second * moment_two + (1.0 - beta_second) * gradient * gradient
    correct_one = 1.0 - beta_first**STEP
    correct_two = 1.0 - beta_second**STEP
    update = (
        moment_one_new / correct_one / (jnp.sqrt(moment_two_new / correct_two) + epsilon)
        + weight_decay * weights
    )
    return (moment_one_new, moment_two_new, weights - learn_rate * update)


def shards(inputs, value_cotangent, master, first_moment, second_moment):
    _, heads, slice_width = master.shape
    head_size = value_cotangent.shape[1] // heads
    head_parts = []
    for head in range(heads):
        head_cot = value_cotangent[:, head * head_size : (head + 1) * head_size]
        head_term = lax.dot_general(
            inputs, head_cot, (((0,), (0,)), ((), ())), preferred_element_type=jnp.float32
        )
        head_parts.append(
            lax.psum_scatter(
                head_term.astype(jnp.bfloat16), "dp", scatter_dimension=1, tiled=True
            ).astype(jnp.float32)
        )
    column_part = jnp.stack(head_parts, axis=1)
    grad_share = lax.psum_scatter(column_part, "fsdp", scatter_dimension=0, tiled=True)
    moment_one_new, moment_two_new, master_new = adam_update(
        grad_share, first_moment, second_moment, master
    )
    narrow_weight = master_new.astype(jnp.bfloat16)
    gathered = lax.all_gather(narrow_weight, "fsdp", axis=0, tiled=True)
    head_index = lax.axis_index("fsdp") % heads
    picked = lax.dynamic_slice_in_dim(gathered, head_index, 1, 1)
    tp_block = picked.reshape(1, gathered.shape[0], slice_width)
    return (moment_one_new, moment_two_new, master_new, tp_block)


VMEM_BYTES = 67043328
SPARE_BYTES = 64 * 1024
PLANE = 8


def step_kernel(
    n, x_hbm, g_hbm, w_hbm, m_hbm, v_hbm, m_out, v_out, w_out, tp_out,
    x_ref, g_ref, w_ref, m_ref, v_ref,
    mate_x, mate_g, total, parts, relay, plane_in, column_part, column_in, blocks,
    load_sem, mate_send, mate_recv, plane_send, plane_recv,
    column_send, column_recv, line_send, line_recv, row_send, row_recv,
):
    me = lax.axis_index("fsdp")
    z = me // PLANE
    q = lax.rem(me, PLANE)
    spot = q // 2
    core = lax.rem(q, 2)
    mate = me + 1 - 2 * core
    spots = PLANE // 2
    depth = n // PLANE
    layers = depth // 2
    rows, heads, head_size = w_ref.shape
    half = x_ref.shape[1] // 2
    tile = half // layers
    both = 2 * rows
    worker = z // layers

    loads = [
        pltpu.make_async_copy(source, target, load_sem.at[i])
        for i, (source, target) in enumerate(
            ((g_hbm, g_ref), (x_hbm, x_ref), (w_hbm, w_ref), (m_hbm, m_ref), (v_hbm, v_ref))
        )
    ]
    for load in loads:
        load.start()

    def to(device):
        return dict(device_id={"fsdp": device}, device_id_type=pl.DeviceIdType.MESH)

    def plane_mate(step):
        return z * PLANE + lax.rem(q + step, PLANE)

    def layer(step):
        return lax.rem(z + step, depth)

    barrier = pltpu.get_barrier_semaphore()
    for step in range(1, PLANE):
        pl.semaphore_signal(barrier, inc=1, **to(plane_mate(step)))
    for step in range(1, depth):
        for side in range(2):
            pl.semaphore_signal(
                barrier, inc=1, **to(layer(step) * PLANE + 2 * spot + side)
            )
    loads[0].wait()
    loads[1].wait()
    pl.semaphore_wait(barrier, PLANE - 1 + 2 * (depth - 1))

    swap_g = pltpu.make_async_remote_copy(
        g_ref, mate_g, mate_send.at[0], mate_recv.at[0], **to(mate)
    )
    swap_x = [
        pltpu.make_async_remote_copy(
            x_ref.at[:, pl.ds(pl.multiple_of((1 - core) * half + t * tile, 128), tile)],
            mate_x.at[:, pl.ds(t * tile, tile)],
            mate_send.at[1 + t], mate_recv.at[1 + t], **to(mate)
        )
        for t in range(layers)
    ]
    swap_g.start()
    for swap in swap_x:
        swap.start()

    def transposed_dot(left, right):
        return lax.dot_general(
            left, right, (((0,), (0,)), ((), ())), preferred_element_type=jnp.float32
        )

    def rows_of_tile(t):
        return slice(t * tile, (t + 1) * tile)

    for t in range(layers):
        own = x_ref[:, pl.ds(pl.multiple_of(core * half + t * tile, 128), tile)]
        total[rows_of_tile(t), :] = transposed_dot(own, g_ref[...])
    swap_g.wait_recv()

    across_x = spot + 1 - 2 * lax.rem(spot, 2)
    across_y = lax.rem(spot + 2, spots)
    across_both = lax.rem(across_x + 2, spots)

    def order_of(t):
        return (across_x, across_y) if t % 2 == 0 else (across_y, across_x)

    def part_rows(t, target):
        return pl.ds(pl.multiple_of(t * tile + target * both, 16), both)

    def plane_copy(phase, t, kind):
        first, second = order_of(t)
        piece = pl.ds(t * both, both)
        if kind == 2:
            source, target = relay.at[phase, piece], second
        else:
            owner = first if kind == 0 else across_both
            source, target = parts.at[phase, part_rows(t, owner)], first
        index = (phase * layers + t) * 3 + kind
        return pltpu.make_async_remote_copy(
            source, plane_in.at[kind, phase, piece],
            plane_send.at[index], plane_recv.at[index],
            **to(z * PLANE + 2 * target + core),
        )

    def plane_start(phase, t):
        plane_copy(phase, t, 1).start()
        plane_copy(phase, t, 0).start()

    for t in range(layers):
        block = rows_of_tile(t)
        swap_x[t].wait_recv()
        summed = (
            total[block, :] + transposed_dot(mate_x[:, block], mate_g[...])
        ).astype(jnp.bfloat16)
        for head in range(heads):
            parts[head, block, :] = summed[:, head * head_size : (head + 1) * head_size]
        plane_start(0, t)
    if heads > 1:
        for t in range(layers):
            plane_start(1, t)

    def plane_relay(phase):
        for t in range(layers):
            piece = slice(t * both, (t + 1) * both)
            plane_copy(phase, t, 1).wait_recv()
            relay[phase, piece, :] = (
                parts[phase, part_rows(t, order_of(t)[1]), :].astype(jnp.float32)
                + plane_in[1, phase, piece, :].astype(jnp.float32)
            ).astype(jnp.bfloat16)
            plane_copy(phase, t, 2).start()
        if phase + 2 < heads:
            for t in range(layers):
                plane_start(phase + 2, t)

    def column_copy(phase, t, side, source):
        index = (phase * layers + t) * 2 + side
        return pltpu.make_async_remote_copy(
            column_part.at[phase, pl.ds(t * both + side * rows, rows)],
            column_in.at[source, phase],
            column_send.at[index],
            column_recv.at[phase * depth + source],
            **to((core * layers + t) * PLANE + 2 * spot + side),
        )

    def is_me(t, side):
        return (core * layers + t) * PLANE + 2 * spot + side == me

    def plane_sum(phase, t):
        piece = slice(t * both, (t + 1) * both)
        plane_copy(phase, t, 0).wait_recv()
        value = parts[phase, part_rows(t, spot), :].astype(jnp.float32) + plane_in[
            0, phase, piece, :
        ].astype(jnp.float32)
        plane_copy(phase, t, 2).wait_recv()
        value = value + plane_in[2, phase, piece, :].astype(jnp.float32)
        column_part[phase, t * both : (t + 1) * both, :] = value.astype(jnp.bfloat16)
        for side in range(2):
            @pl.when(jnp.logical_not(is_me(t, side)))
            def _():
                column_copy(phase, t, side, z).start()

            @pl.when(is_me(t, side))
            def _():
                column_in[z, phase] = column_part[
                    phase, t * both + side * rows : t * both + (side + 1) * rows, :
                ]

    def line_copy(phase, step, source):
        target = layer(step)
        return pltpu.make_async_remote_copy(
            blocks.at[z, phase],
            blocks.at[source, phase],
            line_send.at[phase * depth + target],
            line_recv.at[phase * depth + source],
            **to(target * PLANE + q),
        )

    def rows_of(owner):
        return pl.ds(pl.multiple_of(owner * rows, 16), rows)

    def row_copy(source, target):
        return pltpu.make_async_remote_copy(
            blocks.at[source, lax.rem(target, heads)],
            tp_out.at[0, rows_of(source * PLANE + q)],
            row_send.at[source * PLANE + target],
            row_recv.at[source * PLANE + q],
            **to(z * PLANE + target),
        )

    def spread(phase, source):
        for target in range(phase, PLANE, heads):
            @pl.when(target != q)
            def _():
                row_copy(source, target).start()

            @pl.when(target == q)
            def _():
                tp_out[0, rows_of(source * PLANE + q), :] = blocks[source, phase]

    def update(phase):
        for source in range(depth):
            @pl.when(source * PLANE + 2 * spot + worker != me)
            def _():
                column_copy(phase, 0, 0, source).wait_recv()
        gradient = column_in[0, phase].astype(jnp.float32)
        for source in range(1, depth):
            gradient = gradient + column_in[source, phase].astype(jnp.float32)
        m_new, v_new, w_new = adam_update(
            gradient, m_ref[:, phase, :], v_ref[:, phase, :], w_ref[:, phase, :]
        )
        blocks[z, phase] = w_new.astype(jnp.bfloat16)
        for step in range(depth - 1, 0, -1):
            line_copy(phase, step, z).start()
        spread(phase, z)
        m_out[:, phase, :] = m_new
        v_out[:, phase, :] = v_new
        w_out[:, phase, :] = w_new

    def forward(phase):
        for step in range(1, depth):
            source = layer(step)
            line_copy(phase, step, source).wait_recv()
            spread(phase, source)

    def plane_finish(phase):
        for t in range(layers):
            plane_sum(phase, t)

    events = sorted(
        (start + pace * phase, phase, stage)
        for stage, (start, pace) in enumerate(
            ((3.0, 2.3), (6.1, 2.4), (10.2, 2.4), (15.1, 2.4))
        )
        for phase in range(heads)
    )
    stages = (plane_relay, plane_finish, update, forward)
    waiting = loads[2:]
    for _, phase, stage in events:
        if stages[stage] is update:
            while waiting:
                waiting.pop().wait()
        stages[stage](phase)

    pieces = [(phase, t) for phase in range(heads) for t in range(layers)]
    swap_g.wait_send()
    for swap in swap_x:
        swap.wait_send()
    for phase, t in pieces:
        for kind in range(3):
            plane_copy(phase, t, kind).wait_send()
        for side in range(2):
            @pl.when(jnp.logical_not(is_me(t, side)))
            def _():
                column_copy(phase, t, side, z).wait_send()
    for phase in range(heads):
        for step in range(1, depth):
            line_copy(phase, step, z).wait_send()
    for source in range(depth):
        for step in range(1, PLANE):
            other = lax.rem(q + step, PLANE)
            row_copy(source, other).wait_send()
            pltpu.make_async_remote_copy(
                blocks.at[0, 0], tp_out.at[0, rows_of(source * PLANE + other)],
                row_send.at[0], row_recv.at[source * PLANE + other], **to(mate),
            ).wait_recv()


def finish_kernel(*refs):
    count = (len(refs) - 1) // 2
    copies = [
        pltpu.make_async_copy(refs[i], refs[count + i], refs[-1].at[i])
        for i in range(count)
    ]
    for copy in copies:
        copy.start()
    for copy in copies:
        copy.wait()


def fused(n, inputs, value_cotangent, master, first_moment, second_moment):
    tokens, features = inputs.shape
    width = value_cotangent.shape[1]
    rows, heads, head_size = master.shape
    half = features // 2
    depth = n // PLANE
    layers = depth // 2
    state = jax.ShapeDtypeStruct(master.shape, jnp.float32)
    block = jax.ShapeDtypeStruct((1, features, head_size), jnp.bfloat16)
    results = 12 * master.size + 2 * block.size + SPARE_BYTES
    vmem = pl.BlockSpec(memory_space=pltpu.VMEM)
    narrow = jnp.bfloat16
    held = pl.pallas_call(
        functools.partial(step_kernel, n),
        out_shape=tuple(pltpu.VMEM(a.shape, a.dtype) for a in (state, state, state, block)),
        in_specs=[pl.BlockSpec(memory_space=pltpu.HBM)] * 5,
        out_specs=[vmem] * 4,
        scratch_shapes=[
            pltpu.VMEM((tokens, features), narrow),
            pltpu.VMEM((tokens, width), narrow),
            pltpu.VMEM(master.shape, jnp.float32),
            pltpu.VMEM(master.shape, jnp.float32),
            pltpu.VMEM(master.shape, jnp.float32),
            pltpu.VMEM((tokens, half), narrow),
            pltpu.VMEM((tokens, width), narrow),
            pltpu.VMEM((half, width), jnp.float32),
            pltpu.VMEM((heads, half, head_size), narrow),
            pltpu.VMEM((heads, layers * 2 * rows, head_size), narrow),
            pltpu.VMEM((3, heads, layers * 2 * rows, head_size), narrow),
            pltpu.VMEM((heads, layers * 2 * rows, head_size), narrow),
            pltpu.VMEM((depth, heads, rows, head_size), narrow),
            pltpu.VMEM((depth, heads, rows, head_size), narrow),
            pltpu.SemaphoreType.DMA((5,)),
            pltpu.SemaphoreType.DMA((1 + layers,)),
            pltpu.SemaphoreType.DMA((1 + layers,)),
            pltpu.SemaphoreType.DMA((heads * layers * 3,)),
            pltpu.SemaphoreType.DMA((heads * layers * 3,)),
            pltpu.SemaphoreType.DMA((heads * layers * 2,)),
            pltpu.SemaphoreType.DMA((heads * depth,)),
            pltpu.SemaphoreType.DMA((heads * depth,)),
            pltpu.SemaphoreType.DMA((heads * depth,)),
            pltpu.SemaphoreType.DMA((n,)),
            pltpu.SemaphoreType.DMA((n,)),
        ],
        compiler_params=pltpu.CompilerParams(
            collective_id=0, has_side_effects=True, vmem_limit_bytes=VMEM_BYTES - results
        ),
    )(inputs, value_cotangent, master, first_moment, second_moment)
    return pl.pallas_call(
        finish_kernel,
        out_shape=(state, state, state, block),
        in_specs=[vmem] * 4,
        out_specs=[pl.BlockSpec(memory_space=pltpu.HBM)] * 4,
        scratch_shapes=[pltpu.SemaphoreType.DMA((4,))],
        compiler_params=pltpu.CompilerParams(vmem_limit_bytes=VMEM_BYTES // 2),
    )(*held)


def solution(mesh):
    n = mesh.shape["fsdp"]

    def body(inputs, value_cotangent, master, first_moment, second_moment):
        rows = master.shape[0]
        direct = (
            mesh.shape["dp"] == 1
            and n % (2 * PLANE) == 0
            and inputs.shape[1] % (256 * (n // (2 * PLANE))) == 0
            and rows % 16 == 0
            and PLANE % master.shape[1] == 0
            and master.shape[2] % 128 == 0
        )
        if direct:
            return fused(n, inputs, value_cotangent, master, first_moment, second_moment)
        return shards(inputs, value_cotangent, master, first_moment, second_moment)

    placed = (
        P(("fsdp", "dp"), None),
        P(("fsdp", "dp"), None),
        P("fsdp", None, "dp"),
        P("fsdp", None, "dp"),
        P("fsdp", None, "dp"),
    )
    return jax.shard_map(
        body,
        mesh=mesh,
        in_specs=placed,
        out_specs=(
            P("fsdp", None, "dp"),
            P("fsdp", None, "dp"),
            P("fsdp", None, "dp"),
            P("fsdp", None, "dp"),
        ),
        check_vma=False,
    )
```

```python
import functools

import jax
import jax.numpy as jnp
from jax import lax
from jax.experimental import pallas as pl
from jax.experimental.pallas import tpu as pltpu
from jax.sharding import PartitionSpec as P

STEP = 8


beta_first = 0.9
beta_second = 0.95
learn_rate = 0.001
weight_decay = 0.1
epsilon = 1e-08


def adam_update(gradient, moment_one, moment_two, weights):
    moment_one_new = beta_first * moment_one + (1.0 - beta_first) * gradient
    moment_two_new = beta_second * moment_two + (1.0 - beta_second) * gradient * gradient
    correct_one = 1.0 - beta_first**STEP
    correct_two = 1.0 - beta_second**STEP
    update = (
        moment_one_new / correct_one / (jnp.sqrt(moment_two_new / correct_two) + epsilon)
        + weight_decay * weights
    )
    return (moment_one_new, moment_two_new, weights - learn_rate * update)


def shards(inputs, value_cotangent, master, first_moment, second_moment):
    _, heads, slice_width = master.shape
    head_size = value_cotangent.shape[1] // heads
    head_parts = []
    for head in range(heads):
        head_cot = value_cotangent[:, head * head_size : (head + 1) * head_size]
        head_term = lax.dot_general(
            inputs, head_cot, (((0,), (0,)), ((), ())), preferred_element_type=jnp.float32
        )
        head_parts.append(
            lax.psum_scatter(
                head_term.astype(jnp.bfloat16), "dp", scatter_dimension=1, tiled=True
            ).astype(jnp.float32)
        )
    column_part = jnp.stack(head_parts, axis=1)
    grad_share = lax.psum_scatter(column_part, "fsdp", scatter_dimension=0, tiled=True)
    moment_one_new, moment_two_new, master_new = adam_update(
        grad_share, first_moment, second_moment, master
    )
    narrow_weight = master_new.astype(jnp.bfloat16)
    gathered = lax.all_gather(narrow_weight, "fsdp", axis=0, tiled=True)
    head_index = lax.axis_index("fsdp") % heads
    picked = lax.dynamic_slice_in_dim(gathered, head_index, 1, 1)
    tp_block = picked.reshape(1, gathered.shape[0], slice_width)
    return (moment_one_new, moment_two_new, master_new, tp_block)


VMEM_BYTES = 67043328
SPARE_BYTES = 64 * 1024
PLANE = 8


def step_kernel(
    n, x_hbm, g_hbm, w_hbm, m_hbm, v_hbm, m_out, v_out, w_out, tp_out,
    x_ref, g_ref, w_ref, m_ref, v_ref,
    mate_x, mate_g, total, parts, plane_in, column_part, column_in, blocks,
    load_sem, mate_send, mate_recv, plane_send, plane_recv,
    column_send, column_recv, line_send, line_recv, row_send, row_recv,
):
    me = lax.axis_index("fsdp")
    z = me // PLANE
    q = lax.rem(me, PLANE)
    spot = q // 2
    core = lax.rem(q, 2)
    mate = me + 1 - 2 * core
    spots = PLANE // 2
    depth = n // PLANE
    layers = depth // 2
    rows, heads, head_size = w_ref.shape
    half = x_ref.shape[1] // 2
    tile = half // layers
    both = 2 * rows
    worker = z // layers

    loads = [
        pltpu.make_async_copy(source, target, load_sem.at[i])
        for i, (source, target) in enumerate(
            ((g_hbm, g_ref), (x_hbm, x_ref), (w_hbm, w_ref), (m_hbm, m_ref), (v_hbm, v_ref))
        )
    ]
    for load in loads:
        load.start()

    def to(device):
        return dict(device_id={"fsdp": device}, device_id_type=pl.DeviceIdType.MESH)

    def plane_mate(step):
        return z * PLANE + lax.rem(q + step, PLANE)

    def layer(step):
        return lax.rem(z + step, depth)

    barrier = pltpu.get_barrier_semaphore()
    for step in range(1, n):
        pl.semaphore_signal(barrier, inc=1, **to(lax.rem(me + step, n)))
    loads[0].wait()
    loads[1].wait()
    pl.semaphore_wait(barrier, n - 1)

    swap_g = pltpu.make_async_remote_copy(
        g_ref, mate_g, mate_send.at[0], mate_recv.at[0], **to(mate)
    )
    swap_x = [
        pltpu.make_async_remote_copy(
            x_ref.at[:, pl.ds(pl.multiple_of((1 - core) * half + t * tile, 128), tile)],
            mate_x.at[:, pl.ds(t * tile, tile)],
            mate_send.at[1 + t], mate_recv.at[1 + t], **to(mate)
        )
        for t in range(layers)
    ]
    swap_g.start()
    for swap in swap_x:
        swap.start()

    def transposed_dot(left, right):
        return lax.dot_general(
            left, right, (((0,), (0,)), ((), ())), preferred_element_type=jnp.float32
        )

    def rows_of_tile(t):
        return slice(t * tile, (t + 1) * tile)

    for t in range(layers):
        own = x_ref[:, pl.ds(pl.multiple_of(core * half + t * tile, 128), tile)]
        total[rows_of_tile(t), :] = transposed_dot(own, g_ref[...])
    swap_g.wait_recv()

    def plane_copy(phase, t, step, source):
        index = (phase * layers + t) * spots
        target = lax.rem(spot + step, spots)
        return pltpu.make_async_remote_copy(
            parts.at[
                phase, pl.ds(pl.multiple_of(t * tile + target * both, 16), both)
            ],
            plane_in.at[source, phase, pl.ds(t * both, both)],
            plane_send.at[index + target],
            plane_recv.at[index + source],
            **to(z * PLANE + 2 * target + core),
        )

    for t in range(layers):
        block = rows_of_tile(t)
        swap_x[t].wait_recv()
        summed = (
            total[block, :] + transposed_dot(mate_x[:, block], mate_g[...])
        ).astype(jnp.bfloat16)
        for head in range(heads):
            parts[head, block, :] = summed[:, head * head_size : (head + 1) * head_size]
        for step in range(1, spots):
            plane_copy(0, t, step, spot).start()
    for phase in range(1, heads):
        for t in range(layers):
            for step in range(1, spots):
                plane_copy(phase, t, step, spot).start()

    def column_copy(phase, t, side, source):
        index = (phase * layers + t) * 2 + side
        return pltpu.make_async_remote_copy(
            column_part.at[phase, pl.ds(t * both + side * rows, rows)],
            column_in.at[source, phase],
            column_send.at[index],
            column_recv.at[phase * depth + source],
            **to((core * layers + t) * PLANE + 2 * spot + side),
        )

    def is_me(t, side):
        return (core * layers + t) * PLANE + 2 * spot + side == me

    def plane_sum(phase, t):
        for step in range(1, spots):
            plane_copy(phase, t, step, lax.rem(spot + step, spots)).wait_recv()
        value = parts[
            phase, pl.ds(pl.multiple_of(t * tile + spot * both, 16), both), :
        ].astype(jnp.float32)
        for step in range(1, spots):
            value = value + plane_in[
                lax.rem(spot + step, spots), phase, t * both : (t + 1) * both, :
            ].astype(jnp.float32)
        column_part[phase, t * both : (t + 1) * both, :] = value.astype(jnp.bfloat16)
        for side in range(2):
            @pl.when(jnp.logical_not(is_me(t, side)))
            def _():
                column_copy(phase, t, side, z).start()

            @pl.when(is_me(t, side))
            def _():
                column_in[z, phase] = column_part[
                    phase, t * both + side * rows : t * both + (side + 1) * rows, :
                ]

    def line_copy(phase, step, source):
        target = layer(step)
        return pltpu.make_async_remote_copy(
            blocks.at[z, phase],
            blocks.at[source, phase],
            line_send.at[phase * depth + target],
            line_recv.at[phase * depth + source],
            **to(target * PLANE + q),
        )

    def rows_of(owner):
        return pl.ds(pl.multiple_of(owner * rows, 16), rows)

    def row_copy(source, target):
        return pltpu.make_async_remote_copy(
            blocks.at[source, lax.rem(target, heads)],
            tp_out.at[0, rows_of(source * PLANE + q)],
            row_send.at[source * PLANE + target],
            row_recv.at[source * PLANE + q],
            **to(z * PLANE + target),
        )

    def spread(phase, source):
        for target in range(phase, PLANE, heads):
            @pl.when(target != q)
            def _():
                row_copy(source, target).start()

            @pl.when(target == q)
            def _():
                tp_out[0, rows_of(source * PLANE + q), :] = blocks[source, phase]

    last = heads - 1

    def direct_copy(there, target):
        return pltpu.make_async_remote_copy(
            blocks.at[z, last],
            tp_out.at[0, rows_of(me)],
            row_send.at[there * PLANE + target],
            row_recv.at[me],
            **to(there * PLANE + target),
        )

    def update(phase):
        for source in range(depth):
            @pl.when(source * PLANE + 2 * spot + worker != me)
            def _():
                column_copy(phase, 0, 0, source).wait_recv()
        gradient = column_in[0, phase].astype(jnp.float32)
        for source in range(1, depth):
            gradient = gradient + column_in[source, phase].astype(jnp.float32)
        m_new, v_new, w_new = adam_update(
            gradient, m_ref[:, phase, :], v_ref[:, phase, :], w_ref[:, phase, :]
        )
        blocks[z, phase] = w_new.astype(jnp.bfloat16)
        if phase == last:
            for step in range(depth - 1, -1, -1):
                for target in range(phase, PLANE, heads):
                    if step:
                        direct_copy(layer(step), target).start()
                    else:
                        @pl.when(target != q)
                        def _():
                            direct_copy(z, target).start()

            @pl.when(lax.rem(q, heads) == last)
            def _():
                tp_out[0, rows_of(me), :] = blocks[z, phase]
        else:
            for step in range(depth - 1, 0, -1):
                line_copy(phase, step, z).start()
            spread(phase, z)
        m_out[:, phase, :] = m_new
        v_out[:, phase, :] = v_new
        w_out[:, phase, :] = w_new

    def forward(phase):
        for step in range(1, depth):
            source = layer(step)
            line_copy(phase, step, source).wait_recv()
            spread(phase, source)

    pieces = [(phase, t) for phase in range(heads) for t in range(layers)]
    for phase in range(heads + 2):
        if phase < heads:
            for t in range(layers):
                plane_sum(phase, t)
        if phase == 1:
            for load in loads[2:]:
                load.wait()
        if 0 <= phase - 1 < heads:
            update(phase - 1)
        if 0 <= phase - 3 < last:
            forward(phase - 3)

    swap_g.wait_send()
    for swap in swap_x:
        swap.wait_send()
    for phase, t in pieces:
        for step in range(1, spots):
            plane_copy(phase, t, step, spot).wait_send()
        for side in range(2):
            @pl.when(jnp.logical_not(is_me(t, side)))
            def _():
                column_copy(phase, t, side, z).wait_send()
    for phase in range(last):
        for step in range(1, depth):
            line_copy(phase, step, z).wait_send()
    for source in range(depth):
        for step in range(1, PLANE):
            other = lax.rem(q + step, PLANE)
            row_copy(source, other).wait_send()
            pltpu.make_async_remote_copy(
                blocks.at[0, 0], tp_out.at[0, rows_of(source * PLANE + other)],
                row_send.at[0], row_recv.at[source * PLANE + other], **to(mate),
            ).wait_recv()

    @pl.when(lax.rem(q, heads) == last)
    def _():
        for step in range(1, depth):
            direct_copy(layer(step), q).wait_send()
            pltpu.make_async_remote_copy(
                blocks.at[0, 0], tp_out.at[0, rows_of(layer(step) * PLANE + q)],
                row_send.at[0], row_recv.at[layer(step) * PLANE + q], **to(mate),
            ).wait_recv()


def finish_kernel(*refs):
    count = (len(refs) - 1) // 2
    copies = [
        pltpu.make_async_copy(refs[i], refs[count + i], refs[-1].at[i])
        for i in range(count)
    ]
    for copy in copies:
        copy.start()
    for copy in copies:
        copy.wait()


def fused(n, inputs, value_cotangent, master, first_moment, second_moment):
    tokens, features = inputs.shape
    width = value_cotangent.shape[1]
    rows, heads, head_size = master.shape
    half = features // 2
    depth = n // PLANE
    layers = depth // 2
    spots = PLANE // 2
    state = jax.ShapeDtypeStruct(master.shape, jnp.float32)
    block = jax.ShapeDtypeStruct((1, features, head_size), jnp.bfloat16)
    results = 12 * master.size + 2 * block.size + SPARE_BYTES
    vmem = pl.BlockSpec(memory_space=pltpu.VMEM)
    narrow = jnp.bfloat16
    held = pl.pallas_call(
        functools.partial(step_kernel, n),
        out_shape=tuple(pltpu.VMEM(a.shape, a.dtype) for a in (state, state, state, block)),
        in_specs=[pl.BlockSpec(memory_space=pltpu.HBM)] * 5,
        out_specs=[vmem] * 4,
        scratch_shapes=[
            pltpu.VMEM((tokens, features), narrow),
            pltpu.VMEM((tokens, width), narrow),
            pltpu.VMEM(master.shape, jnp.float32),
            pltpu.VMEM(master.shape, jnp.float32),
            pltpu.VMEM(master.shape, jnp.float32),
            pltpu.VMEM((tokens, half), narrow),
            pltpu.VMEM((tokens, width), narrow),
            pltpu.VMEM((half, width), jnp.float32),
            pltpu.VMEM((heads, half, head_size), narrow),
            pltpu.VMEM((spots, heads, layers * 2 * rows, head_size), narrow),
            pltpu.VMEM((heads, layers * 2 * rows, head_size), narrow),
            pltpu.VMEM((depth, heads, rows, head_size), narrow),
            pltpu.VMEM((depth, heads, rows, head_size), narrow),
            pltpu.SemaphoreType.DMA((5,)),
            pltpu.SemaphoreType.DMA((1 + layers,)),
            pltpu.SemaphoreType.DMA((1 + layers,)),
            pltpu.SemaphoreType.DMA((heads * layers * spots,)),
            pltpu.SemaphoreType.DMA((heads * layers * spots,)),
            pltpu.SemaphoreType.DMA((heads * layers * 2,)),
            pltpu.SemaphoreType.DMA((heads * depth,)),
            pltpu.SemaphoreType.DMA((heads * depth,)),
            pltpu.SemaphoreType.DMA((heads * depth,)),
            pltpu.SemaphoreType.DMA((n,)),
            pltpu.SemaphoreType.DMA((n,)),
        ],
        compiler_params=pltpu.CompilerParams(
            collective_id=0, has_side_effects=True, vmem_limit_bytes=VMEM_BYTES - results
        ),
    )(inputs, value_cotangent, master, first_moment, second_moment)
    return pl.pallas_call(
        finish_kernel,
        out_shape=(state, state, state, block),
        in_specs=[vmem] * 4,
        out_specs=[pl.BlockSpec(memory_space=pltpu.HBM)] * 4,
        scratch_shapes=[pltpu.SemaphoreType.DMA((4,))],
        compiler_params=pltpu.CompilerParams(vmem_limit_bytes=VMEM_BYTES // 2),
    )(*held)


def solution(mesh):
    n = mesh.shape["fsdp"]

    def body(inputs, value_cotangent, master, first_moment, second_moment):
        rows = master.shape[0]
        direct = (
            mesh.shape["dp"] == 1
            and n % (2 * PLANE) == 0
            and inputs.shape[1] % (256 * (n // (2 * PLANE))) == 0
            and rows % 16 == 0
            and PLANE % master.shape[1] == 0
            and master.shape[2] % 128 == 0
        )
        if direct:
            return fused(n, inputs, value_cotangent, master, first_moment, second_moment)
        return shards(inputs, value_cotangent, master, first_moment, second_moment)

    placed = (
        P(("fsdp", "dp"), None),
        P(("fsdp", "dp"), None),
        P("fsdp", None, "dp"),
        P("fsdp", None, "dp"),
        P("fsdp", None, "dp"),
    )
    return jax.shard_map(
        body,
        mesh=mesh,
        in_specs=placed,
        out_specs=(
            P("fsdp", None, "dp"),
            P("fsdp", None, "dp"),
            P("fsdp", None, "dp"),
            P("fsdp", None, "dp"),
        ),
        check_vma=False,
    )
```

```python
import functools

import jax
import jax.numpy as jnp
from jax import lax
from jax.experimental import pallas as pl
from jax.experimental.pallas import tpu as pltpu
from jax.sharding import PartitionSpec as P

STEP = 8


beta_first = 0.9
beta_second = 0.95
learn_rate = 0.001
weight_decay = 0.1
epsilon = 1e-08


def adam_update(gradient, moment_one, moment_two, weights):
    moment_one_new = beta_first * moment_one + (1.0 - beta_first) * gradient
    moment_two_new = beta_second * moment_two + (1.0 - beta_second) * gradient * gradient
    correct_one = 1.0 - beta_first**STEP
    correct_two = 1.0 - beta_second**STEP
    update = (
        moment_one_new / correct_one / (jnp.sqrt(moment_two_new / correct_two) + epsilon)
        + weight_decay * weights
    )
    return (moment_one_new, moment_two_new, weights - learn_rate * update)


def shards(inputs, value_cotangent, master, first_moment, second_moment):
    _, heads, slice_width = master.shape
    head_size = value_cotangent.shape[1] // heads
    head_parts = []
    for head in range(heads):
        head_cot = value_cotangent[:, head * head_size : (head + 1) * head_size]
        head_term = lax.dot_general(
            inputs, head_cot, (((0,), (0,)), ((), ())), preferred_element_type=jnp.float32
        )
        head_parts.append(
            lax.psum_scatter(
                head_term.astype(jnp.bfloat16), "dp", scatter_dimension=1, tiled=True
            ).astype(jnp.float32)
        )
    column_part = jnp.stack(head_parts, axis=1)
    grad_share = lax.psum_scatter(column_part, "fsdp", scatter_dimension=0, tiled=True)
    moment_one_new, moment_two_new, master_new = adam_update(
        grad_share, first_moment, second_moment, master
    )
    narrow_weight = master_new.astype(jnp.bfloat16)
    gathered = lax.all_gather(narrow_weight, "fsdp", axis=0, tiled=True)
    head_index = lax.axis_index("fsdp") % heads
    picked = lax.dynamic_slice_in_dim(gathered, head_index, 1, 1)
    tp_block = picked.reshape(1, gathered.shape[0], slice_width)
    return (moment_one_new, moment_two_new, master_new, tp_block)


VMEM_BYTES = 67043328
SPARE_BYTES = 64 * 1024
PLANE = 8


def step_kernel(
    n, x_hbm, g_hbm, w_hbm, m_hbm, v_hbm, m_out, v_out, w_out, tp_out,
    x_ref, g_ref, w_ref, m_ref, v_ref,
    mate_x, mate_g, total, parts, plane_in, column_part, column_in, blocks,
    load_sem, mate_send, mate_recv, plane_send, plane_recv,
    column_send, column_recv, line_send, line_recv, row_send, row_recv,
):
    me = lax.axis_index("fsdp")
    z = me // PLANE
    q = lax.rem(me, PLANE)
    spot = q // 2
    core = lax.rem(q, 2)
    mate = me + 1 - 2 * core
    spots = PLANE // 2
    depth = n // PLANE
    layers = depth // 2
    rows, heads, head_size = w_ref.shape
    half = x_ref.shape[1] // 2
    tile = half // layers
    both = 2 * rows
    worker = z // layers

    loads = [
        pltpu.make_async_copy(source, target, load_sem.at[i])
        for i, (source, target) in enumerate(
            ((g_hbm, g_ref), (x_hbm, x_ref), (w_hbm, w_ref), (m_hbm, m_ref), (v_hbm, v_ref))
        )
    ]
    for load in loads:
        load.start()

    def to(device):
        return dict(device_id={"fsdp": device}, device_id_type=pl.DeviceIdType.MESH)

    def plane_mate(step):
        return z * PLANE + lax.rem(q + step, PLANE)

    def layer(step):
        return lax.rem(z + step, depth)

    barrier = pltpu.get_barrier_semaphore()
    for step in range(1, PLANE):
        pl.semaphore_signal(barrier, inc=1, **to(plane_mate(step)))
    for step in range(1, depth):
        for side in range(2):
            pl.semaphore_signal(
                barrier, inc=1, **to(layer(step) * PLANE + 2 * spot + side)
            )
    loads[0].wait()
    loads[1].wait()
    pl.semaphore_wait(barrier, PLANE - 1 + 2 * (depth - 1))

    swap_g = pltpu.make_async_remote_copy(
        g_ref, mate_g, mate_send.at[0], mate_recv.at[0], **to(mate)
    )
    swap_x = [
        pltpu.make_async_remote_copy(
            x_ref.at[:, pl.ds(pl.multiple_of((1 - core) * half + t * tile, 128), tile)],
            mate_x.at[:, pl.ds(t * tile, tile)],
            mate_send.at[1 + t], mate_recv.at[1 + t], **to(mate)
        )
        for t in range(layers)
    ]
    swap_g.start()
    for swap in swap_x:
        swap.start()

    def transposed_dot(left, right):
        return lax.dot_general(
            left, right, (((0,), (0,)), ((), ())), preferred_element_type=jnp.float32
        )

    def rows_of_tile(t):
        return slice(t * tile, (t + 1) * tile)

    for t in range(layers):
        own = x_ref[:, pl.ds(pl.multiple_of(core * half + t * tile, 128), tile)]
        total[rows_of_tile(t), :] = transposed_dot(own, g_ref[...])
    swap_g.wait_recv()

    def plane_copy(phase, t, step, source):
        index = (phase * layers + t) * spots
        target = lax.rem(spot + step, spots)
        return pltpu.make_async_remote_copy(
            parts.at[
                phase, pl.ds(pl.multiple_of(t * tile + target * both, 16), both)
            ],
            plane_in.at[source, phase, pl.ds(t * both, both)],
            plane_send.at[index + target],
            plane_recv.at[index + source],
            **to(z * PLANE + 2 * target + core),
        )

    for t in range(layers):
        block = rows_of_tile(t)
        swap_x[t].wait_recv()
        summed = (
            total[block, :] + transposed_dot(mate_x[:, block], mate_g[...])
        ).astype(jnp.bfloat16)
        for head in range(heads):
            parts[head, block, :] = summed[:, head * head_size : (head + 1) * head_size]
        for step in range(1, spots):
            plane_copy(0, t, step, spot).start()
    for phase in range(1, heads):
        for t in range(layers):
            for step in range(1, spots):
                plane_copy(phase, t, step, spot).start()

    def column_copy(phase, t, side, source):
        index = (phase * layers + t) * 2 + side
        return pltpu.make_async_remote_copy(
            column_part.at[phase, pl.ds(t * both + side * rows, rows)],
            column_in.at[source, phase],
            column_send.at[index],
            column_recv.at[phase * depth + source],
            **to((core * layers + t) * PLANE + 2 * spot + side),
        )

    def is_me(t, side):
        return (core * layers + t) * PLANE + 2 * spot + side == me

    def plane_sum(phase, t):
        for step in range(1, spots):
            plane_copy(phase, t, step, lax.rem(spot + step, spots)).wait_recv()
        value = parts[
            phase, pl.ds(pl.multiple_of(t * tile + spot * both, 16), both), :
        ].astype(jnp.float32)
        for step in range(1, spots):
            value = value + plane_in[
                lax.rem(spot + step, spots), phase, t * both : (t + 1) * both, :
            ].astype(jnp.float32)
        column_part[phase, t * both : (t + 1) * both, :] = value.astype(jnp.bfloat16)
        for side in range(2):
            @pl.when(jnp.logical_not(is_me(t, side)))
            def _():
                column_copy(phase, t, side, z).start()

            @pl.when(is_me(t, side))
            def _():
                column_in[z, phase] = column_part[
                    phase, t * both + side * rows : t * both + (side + 1) * rows, :
                ]

    def line_copy(phase, step, source):
        target = layer(step)
        return pltpu.make_async_remote_copy(
            blocks.at[z, phase],
            blocks.at[source, phase],
            line_send.at[phase * depth + target],
            line_recv.at[phase * depth + source],
            **to(target * PLANE + q),
        )

    def rows_of(owner):
        return pl.ds(pl.multiple_of(owner * rows, 16), rows)

    def row_copy(source, target):
        return pltpu.make_async_remote_copy(
            blocks.at[source, lax.rem(target, heads)],
            tp_out.at[0, rows_of(source * PLANE + q)],
            row_send.at[source * PLANE + target],
            row_recv.at[source * PLANE + q],
            **to(z * PLANE + target),
        )

    def spread(phase, source):
        for target in range(phase, PLANE, heads):
            @pl.when(target != q)
            def _():
                row_copy(source, target).start()

            @pl.when(target == q)
            def _():
                tp_out[0, rows_of(source * PLANE + q), :] = blocks[source, phase]

    def update(phase):
        for source in range(depth):
            @pl.when(source * PLANE + 2 * spot + worker != me)
            def _():
                column_copy(phase, 0, 0, source).wait_recv()
        gradient = column_in[0, phase].astype(jnp.float32)
        for source in range(1, depth):
            gradient = gradient + column_in[source, phase].astype(jnp.float32)
        m_new, v_new, w_new = adam_update(
            gradient, m_ref[:, phase, :], v_ref[:, phase, :], w_ref[:, phase, :]
        )
        blocks[z, phase] = w_new.astype(jnp.bfloat16)
        for step in range(depth - 1, 0, -1):
            line_copy(phase, step, z).start()
        spread(phase, z)
        m_out[:, phase, :] = m_new
        v_out[:, phase, :] = v_new
        w_out[:, phase, :] = w_new

    def forward(phase):
        for step in range(1, depth):
            source = layer(step)
            line_copy(phase, step, source).wait_recv()
            spread(phase, source)

    pieces = [(phase, t) for phase in range(heads) for t in range(layers)]
    for phase in range(heads + 3):
        if phase < heads:
            for t in range(layers):
                plane_sum(phase, t)
        if phase == 1:
            for load in loads[2:]:
                load.wait()
        if 0 <= phase - 1 < heads:
            update(phase - 1)
        if 0 <= phase - 3 < heads:
            forward(phase - 3)
    swap_g.wait_send()
    for swap in swap_x:
        swap.wait_send()
    for phase, t in pieces:
        for step in range(1, spots):
            plane_copy(phase, t, step, spot).wait_send()
        for side in range(2):
            @pl.when(jnp.logical_not(is_me(t, side)))
            def _():
                column_copy(phase, t, side, z).wait_send()
    for phase in range(heads):
        for step in range(1, depth):
            line_copy(phase, step, z).wait_send()
    for source in range(depth):
        for step in range(1, PLANE):
            other = lax.rem(q + step, PLANE)
            row_copy(source, other).wait_send()
            pltpu.make_async_remote_copy(
                blocks.at[0, 0], tp_out.at[0, rows_of(source * PLANE + other)],
                row_send.at[0], row_recv.at[source * PLANE + other], **to(mate),
            ).wait_recv()


def finish_kernel(*refs):
    count = (len(refs) - 1) // 2
    copies = [
        pltpu.make_async_copy(refs[i], refs[count + i], refs[-1].at[i])
        for i in range(count)
    ]
    for copy in copies:
        copy.start()
    for copy in copies:
        copy.wait()


def fused(n, inputs, value_cotangent, master, first_moment, second_moment):
    tokens, features = inputs.shape
    width = value_cotangent.shape[1]
    rows, heads, head_size = master.shape
    half = features // 2
    depth = n // PLANE
    layers = depth // 2
    spots = PLANE // 2
    state = jax.ShapeDtypeStruct(master.shape, jnp.float32)
    block = jax.ShapeDtypeStruct((1, features, head_size), jnp.bfloat16)
    results = 12 * master.size + 2 * block.size + SPARE_BYTES
    vmem = pl.BlockSpec(memory_space=pltpu.VMEM)
    narrow = jnp.bfloat16
    held = pl.pallas_call(
        functools.partial(step_kernel, n),
        out_shape=tuple(pltpu.VMEM(a.shape, a.dtype) for a in (state, state, state, block)),
        in_specs=[pl.BlockSpec(memory_space=pltpu.HBM)] * 5,
        out_specs=[vmem] * 4,
        scratch_shapes=[
            pltpu.VMEM((tokens, features), narrow),
            pltpu.VMEM((tokens, width), narrow),
            pltpu.VMEM(master.shape, jnp.float32),
            pltpu.VMEM(master.shape, jnp.float32),
            pltpu.VMEM(master.shape, jnp.float32),
            pltpu.VMEM((tokens, half), narrow),
            pltpu.VMEM((tokens, width), narrow),
            pltpu.VMEM((half, width), jnp.float32),
            pltpu.VMEM((heads, half, head_size), narrow),
            pltpu.VMEM((spots, heads, layers * 2 * rows, head_size), narrow),
            pltpu.VMEM((heads, layers * 2 * rows, head_size), narrow),
            pltpu.VMEM((depth, heads, rows, head_size), narrow),
            pltpu.VMEM((depth, heads, rows, head_size), narrow),
            pltpu.SemaphoreType.DMA((5,)),
            pltpu.SemaphoreType.DMA((1 + layers,)),
            pltpu.SemaphoreType.DMA((1 + layers,)),
            pltpu.SemaphoreType.DMA((heads * layers * spots,)),
            pltpu.SemaphoreType.DMA((heads * layers * spots,)),
            pltpu.SemaphoreType.DMA((heads * layers * 2,)),
            pltpu.SemaphoreType.DMA((heads * depth,)),
            pltpu.SemaphoreType.DMA((heads * depth,)),
            pltpu.SemaphoreType.DMA((heads * depth,)),
            pltpu.SemaphoreType.DMA((n,)),
            pltpu.SemaphoreType.DMA((n,)),
        ],
        compiler_params=pltpu.CompilerParams(
            collective_id=0, has_side_effects=True, vmem_limit_bytes=VMEM_BYTES - results
        ),
    )(inputs, value_cotangent, master, first_moment, second_moment)
    return pl.pallas_call(
        finish_kernel,
        out_shape=(state, state, state, block),
        in_specs=[vmem] * 4,
        out_specs=[pl.BlockSpec(memory_space=pltpu.HBM)] * 4,
        scratch_shapes=[pltpu.SemaphoreType.DMA((4,))],
        compiler_params=pltpu.CompilerParams(vmem_limit_bytes=VMEM_BYTES // 2),
    )(*held)


def solution(mesh):
    n = mesh.shape["fsdp"]

    def body(inputs, value_cotangent, master, first_moment, second_moment):
        rows = master.shape[0]
        direct = (
            mesh.shape["dp"] == 1
            and n % (2 * PLANE) == 0
            and inputs.shape[1] % (256 * (n // (2 * PLANE))) == 0
            and rows % 16 == 0
            and PLANE % master.shape[1] == 0
            and master.shape[2] % 128 == 0
        )
        if direct:
            return fused(n, inputs, value_cotangent, master, first_moment, second_moment)
        return shards(inputs, value_cotangent, master, first_moment, second_moment)

    placed = (
        P(("fsdp", "dp"), None),
        P(("fsdp", "dp"), None),
        P("fsdp", None, "dp"),
        P("fsdp", None, "dp"),
        P("fsdp", None, "dp"),
    )
    return jax.shard_map(
        body,
        mesh=mesh,
        in_specs=placed,
        out_specs=(
            P("fsdp", None, "dp"),
            P("fsdp", None, "dp"),
            P("fsdp", None, "dp"),
            P("fsdp", None, "dp"),
        ),
        check_vma=False,
    )
```
